32 devices in a mesh: task: 4 (over z), mp: 8 (over y, x, core).
Axes of the slice: x: 2, y: 2, z: 4, core: 2. Of those that a mesh axis runs over, the one named last changes fastest.
Arguments:
- deter: float32 [1024, 4096], P('task', 'mp'), may hold values from -3 to 3
- draws: int32 [4, 32, 1024], P(None, None, 'task'), may hold values from 0 to 31
- actions: int32 [4, 1024], P(None, 'task'), may hold values from 0 to 17
- horizons: int32 [64], replicated, may hold values from 5 to 30, as said below
- offsets: int32 [4, 4], replicated, may hold values from 0 to 3, as said below
- embed_stoch: bfloat16 [1024, 1024], replicated, may hold values from -1 to 1
- embed_act: bfloat16 [18, 1024], replicated, may hold values from -6 to 6
- gru_weight: bfloat16 [5120, 3, 4096], P(None, None, 'mp'), may hold values from -0.078125 to 0.078125
- prior_weight: bfloat16 [4096, 1024], replicated, may hold values from -0.09375 to 0.09375
- logit_weight: bfloat16 [1024, 1024], replicated, may hold values from -0.75 to 0.75
- head_weight: bfloat16 [1024, 2], replicated, may hold values from -0.375 to 0.375
Outputs:
- log_prob: float32 [4, 1024], P(None, 'task')
- reward: float32 [4, 1024], P(None, 'task')
- continuation: float32 [4, 1024], P(None, 'task')
- final_deter: float32 [1024, 4096], P('task', 'mp')
The draws below stay inside these ranges and needn't reach their ends.
Inputs may be any that keep to these rules, and one draw needn't show every extreme that they name: `horizons`: rows of task k are home rows k * (16) up to (k + 1) * 16 - 1. `offsets`: the 4 numbers of one row are distinct.
All inputs are finite; a program needn't handle non-finite values.
Results may differ from the reference program's by a relative error of at most 0.0045.
Values may be sent and summed in bfloat16 or wider, within the bound.
A program may use at most 128 MiB of HBM per device.

```python
import jax
import jax.numpy as jnp
from jax import lax

DET = 4096
HID = 1024
GROUPS = 32
CLASSES = 32
ACTS = 18
TASKS = 64
BLK_DEV = 4
BROWS = 64
STEPS = 4
WSTART = 16
STOCH = 1024
BLOCKS = 16
ROWS = 1024
N_TASK = 4


def plan_helper(key):
    horizon_key = jax.random.fold_in(key, 11)
    horizons = jax.random.randint(horizon_key, (TASKS,), 5, 31).astype(jnp.int32)
    holders = BLOCKS // BLK_DEV
    per_task = BLOCKS * BROWS // TASKS
    row_task = jnp.arange(BLOCKS * BROWS, dtype=jnp.int32) // per_task
    places = jnp.arange(holders, dtype=jnp.int32)[:, None]
    local_slot = jnp.arange(BLK_DEV, dtype=jnp.int32)[None, :]
    running = jnp.zeros((BLK_DEV,), jnp.int32)
    shift_rows = []
    for moment in range(STEPS):
        live_rows = (horizons[row_task] > WSTART + moment).astype(jnp.int32)
        live_blocks = jnp.max(live_rows.reshape(BLOCKS, BROWS), axis=1).reshape(holders, BLK_DEV)
        moment_key = jax.random.fold_in(jax.random.fold_in(key, 23), moment)
        candidates = []
        heaviest = []
        for option in range(16):
            shifts = jax.random.permutation(jax.random.fold_in(moment_key, option), holders)[:BLK_DEV].astype(jnp.int32)
            landing = (running + shifts) % holders
            source = (places - landing[None, :]) % holders
            slot_live = live_blocks[source, local_slot]
            heaviest.append(jnp.max(jnp.sum(slot_live, axis=1)))
            candidates.append(shifts)
        chosen = jnp.argmin(jnp.stack(heaviest))
        shifts = jnp.stack(candidates)[chosen]
        running = (running + shifts) % holders
        shift_rows.append(shifts)
    return (horizons, jnp.stack(shift_rows).astype(jnp.int32))


def draw_horizons(key, part):
    return plan_helper(key)[0]


def draw_offsets(key, part):
    return plan_helper(key)[1]


def set_ends(array, stream_key, smallest, high):
    shape = array.shape
    index_at = [jax.random.randint(jax.random.fold_in(stream_key, axis), (), 0, shape[axis]) for axis in range(len(shape))]
    array = array.at[tuple(index_at)].set(smallest)
    longest = shape.index(max(shape))
    index_at[longest] = (index_at[longest] + 1) % shape[longest]
    return array.at[tuple(index_at)].set(high)


def level_of(stream_key, dims, pieces, smallest, high):
    factor_of = 1.0
    for axis_at, blocks in pieces:
        steps = jax.random.uniform(jax.random.fold_in(jax.random.fold_in(stream_key, 6), axis_at), (blocks,), jnp.float32, smallest / len(pieces), high / len(pieces))
        factor_of = factor_of * jnp.repeat(jnp.exp(steps), dims[axis_at] // blocks).reshape((-1,) + (1,) * (len(dims) - 1 - axis_at))
    return factor_of


def normal_values(stream_key, shape, deviation, limit, cuts=(), held_as=jnp.bfloat16):
    factor_of = level_of(stream_key, shape, cuts, -0.22, 0.18) if cuts else 1.0
    values = jax.random.normal(stream_key, shape, jnp.float32) * deviation * factor_of
    return jnp.minimum(jnp.maximum(values, -limit), limit).astype(held_as)


def setup_inputs(seed: int = 0) -> dict:
    arg_keys = jax.random.split(jax.random.key(seed), 12)
    deter = normal_values(arg_keys[0], (ROWS, DET), 0.5, 3.0, ((0, 4), (1, 8)), jnp.float32)
    draws = set_ends(jax.random.randint(arg_keys[1], (STEPS, GROUPS, ROWS), 0, CLASSES), jax.random.fold_in(arg_keys[1], 1), 0, CLASSES - 1).astype(jnp.int32)
    actions = set_ends(jax.random.randint(arg_keys[2], (STEPS, ROWS), 0, ACTS), jax.random.fold_in(arg_keys[2], 1), 0, ACTS - 1).astype(jnp.int32)
    horizons = draw_horizons(jax.random.fold_in(arg_keys[11], 71), 0)
    offsets = draw_offsets(jax.random.fold_in(arg_keys[11], 71), 0)
    embed_stoch = normal_values(arg_keys[5], (STOCH, HID), GROUPS ** -0.5, 1.0)
    embed_act = normal_values(arg_keys[6], (ACTS, HID), 1.0, 6.0)
    gru_weight = normal_values(arg_keys[7], (HID + DET, 3, DET), (HID + DET) ** -0.5, 0.078125, ((2, 8),))
    prior_weight = normal_values(arg_keys[8], (DET, HID), DET ** -0.5, 0.09375)
    logit_weight = normal_values(arg_keys[9], (HID, STOCH), (HID // 16) ** -0.5, 0.75)
    head_weight = normal_values(arg_keys[10], (HID, 2), (HID // 4) ** -0.5, 0.375)
    return {"deter": deter, "draws": draws, "actions": actions, "horizons": horizons, "offsets": offsets, "embed_stoch": embed_stoch, "embed_act": embed_act, "gru_weight": gru_weight, "prior_weight": prior_weight, "logit_weight": logit_weight, "head_weight": head_weight}


def layer_norm(values):
    average = lax.optimization_barrier(jnp.mean(values, axis=-1, keepdims=True))
    squares = lax.optimization_barrier(jnp.mean(values * values, axis=-1, keepdims=True))
    return (values - average) * lax.rsqrt(squares - average * average + 1e-05)

def reference(deter, draws, actions, horizons, offsets, embed_stoch, embed_act, gru_weight, prior_weight, logit_weight, head_weight):
    rows_total = deter.shape[0]
    per_task = rows_total // TASKS
    holders = N_TASK
    places = jnp.arange(holders, dtype=jnp.int32)[:, None]
    local_slot = jnp.arange(BLK_DEV, dtype=jnp.int32)[None, :]
    within = jnp.arange(BROWS, dtype=jnp.int32)
    classes = jnp.arange(CLASSES, dtype=jnp.int32)
    action_ids = jnp.arange(ACTS, dtype=jnp.int32)
    gate_matrix = gru_weight.reshape(HID + DET, 3 * DET)
    carried = deter
    running = jnp.zeros((BLK_DEV,), jnp.int32)
    logp_list, reward_list, cont_list = ([], [], [])
    for moment in range(STEPS):
        offset_now = offsets[moment].astype(jnp.int32)
        source = ((places - offset_now[None, :]) % holders).astype(jnp.int32)
        carried = carried.reshape(holders, BLK_DEV, BROWS, DET)[source, local_slot].reshape(rows_total, DET)
        running = (running + offset_now) % holders
        home_block = (places - running[None, :]) % holders * BLK_DEV + local_slot
        home_rows = (home_block[:, :, None] * BROWS + within).reshape(rows_total).astype(jnp.int32)
        living = (horizons[home_rows // per_task] > WSTART + moment).astype(jnp.float32)
        chosen_hot = (jnp.transpose(draws[moment])[:, :, None] == classes).astype(jnp.float32)
        stoch_hot = chosen_hot.astype(jnp.bfloat16).reshape(rows_total, STOCH)
        action_hot = (actions[moment][:, None] == action_ids[None, :]).astype(jnp.bfloat16)
        carried_low = carried.astype(jnp.bfloat16)
        embed_pre = jnp.dot(stoch_hot, embed_stoch, preferred_element_type=jnp.float32) + jnp.dot(action_hot, embed_act, preferred_element_type=jnp.float32)
        embedded = jax.nn.silu(layer_norm(embed_pre)).astype(jnp.bfloat16)
        joined = jnp.concatenate([embedded, carried_low], axis=1)
        gate_parts = jnp.dot(joined, gate_matrix, preferred_element_type=jnp.float32)
        normed = layer_norm(gate_parts).reshape(rows_total, 3, DET)
        reset_gate = jax.nn.sigmoid(normed[:, 0])
        candidate = jnp.tanh(reset_gate * normed[:, 1])
        update = jax.nn.sigmoid(normed[:, 2] - 1.0)
        renewed = update * candidate + (1.0 - update) * carried
        prior_pre = jnp.dot(carried_low, prior_weight, preferred_element_type=jnp.float32)
        hidden = jax.nn.silu(layer_norm(prior_pre)).astype(jnp.bfloat16)
        raw_logits = jnp.dot(hidden, logit_weight, preferred_element_type=jnp.float32).reshape(rows_total, GROUPS, CLASSES)
        capped = 5.0 * jnp.tanh(raw_logits / 5.0)
        exponent = jnp.exp(capped)
        chances = 0.99 * exponent / lax.optimization_barrier(jnp.sum(exponent, axis=-1, keepdims=True)) + 0.01 / CLASSES
        log_prob = lax.optimization_barrier(jnp.sum(jnp.log(lax.optimization_barrier(jnp.sum(chances * chosen_hot, axis=-1))), axis=-1)) * living
        head_out = jnp.dot(hidden, head_weight, preferred_element_type=jnp.float32)
        logp_list.append(log_prob)
        reward_list.append(head_out[:, 0] * living)
        cont_list.append(jax.nn.sigmoid(head_out[:, 1]) * living)
        carried = jnp.where(living[:, None] > 0, renewed, carried)
    return (jnp.stack(logp_list), jnp.stack(reward_list), jnp.stack(cont_list), carried)
```

```python
import functools

import jax
import jax.numpy as jnp
from jax import lax
from jax.experimental import pallas as pl
from jax.experimental.pallas import tpu as pltpu
from jax.sharding import PartitionSpec as P

HID = 1024
GROUPS = 32
CLASSES = 32
ACTS = 18
TASKS = 64
BLK_DEV = 4
STEPS = 4
WSTART = 16
LANES = 128
PACKED = 40


def normed_rows(values):
    entries = values.shape[-1]
    average = jnp.sum(values, axis=-1, keepdims=True) / entries
    squares = jnp.sum(values * values, axis=-1, keepdims=True) / entries
    return (values - average) * lax.rsqrt(squares - average * average + 1e-05)


def product(rows_in, weight):
    return jnp.dot(rows_in, weight, preferred_element_type=jnp.float32)


def product_nt(rows_in, weight):
    return lax.dot_general(
        rows_in, weight, (((1,), (1,)), ((), ())), preferred_element_type=jnp.float32
    )


def flipped(index, mask):
    bit = 1
    while bit <= mask:
        if mask & bit:
            index = index + bit * (1 - 2 * ((index // bit) % 2))
        bit *= 2
    return index


def window_kernel(
    holders,
    shards,
    groups,
    rows,
    share,
    horizons_ref,
    offsets_ref,
    actions_ref,
    act_ref,
    head_ref,
    deter_ref,
    draws_ref,
    stoch_ref,
    weight_ref,
    prior_ref,
    logit_ref,
    log_prob_ref,
    reward_ref,
    continuation_ref,
    final_ref,
    carried,
    draws,
    act,
    stoch,
    weight,
    prior,
    logit,
    packed,
    spread,
    classes_of,
    embedded,
    horizon,
    own_states,
    own_classes,
    wide,
    hidden,
    gath,
    parts,
    stats,
    leaving,
    passing,
    routed,
    landed,
    found,
    settled,
    fetch_sem,
    send_sem,
    recv_sem,
    stat_send,
    stat_recv,
    pack_send,
    pack_recv,
    leave_send,
    leave_recv,
    route_send,
    route_recv,
    found_send,
    found_recv,
    settled_send,
    settled_recv,
):
    me = lax.axis_index("mp")
    place = lax.axis_index("task")
    peers = {mask: flipped(me, mask) for mask in range(1, shards)}
    rows_here = groups * rows
    block_rows = rows_here // BLK_DEV
    group_blocks = BLK_DEV // groups
    piece = block_rows // holders
    own_rows = rows_here // shards
    padded = own_states.shape[0]
    tasks_here = TASKS // holders
    task_rows = rows_here // tasks_here

    def fetch(k, source_ref, target):
        return pltpu.make_async_copy(source_ref, target, fetch_sem.at[k])

    fetches = [
        fetch(0, draws_ref, draws),
        fetch(1, deter_ref, carried),
        fetch(2, stoch_ref, stoch),
        fetch(3, weight_ref, weight),
        fetch(4, prior_ref, prior),
        fetch(5, logit_ref, logit),
    ]
    for k in range(4):
        fetches[k].start()
    barrier = pltpu.get_barrier_semaphore()

    def ahead_of(ahead):
        return lax.rem(place + ahead, holders)

    for mask in range(1, shards):
        pl.semaphore_signal(
            barrier,
            inc=1,
            device_id={"mp": peers[mask]},
            device_id_type=pl.DeviceIdType.MESH,
        )
    for ahead in range(1, holders):
        pl.semaphore_signal(
            barrier,
            inc=1,
            device_id={"task": ahead_of(ahead)},
            device_id_type=pl.DeviceIdType.MESH,
        )

    def across(source_ref, target_ref, send, recv, ahead):
        return pltpu.make_async_remote_copy(
            src_ref=source_ref,
            dst_ref=target_ref,
            send_sem=send,
            recv_sem=recv,
            device_id={"task": ahead_of(ahead)},
            device_id_type=pl.DeviceIdType.MESH,
        )

    def pack_copy(t, ahead, slot):
        return across(
            packed.at[place, t],
            packed.at[slot, t],
            pack_send.at[t, ahead],
            pack_recv.at[t, ahead],
            ahead,
        )

    def leave_copy(g, ahead):
        return across(
            leaving.at[g, ahead_of(ahead)],
            passing.at[g, place],
            leave_send.at[g, ahead],
            leave_recv.at[g, ahead],
            ahead,
        )

    def route_copy(g, ahead):
        return across(
            routed.at[g, ahead_of(ahead)],
            landed.at[g, place],
            route_send.at[g, ahead],
            route_recv.at[g, ahead],
            ahead,
        )

    def found_copy(ahead):
        return across(
            found.at[place], found.at[place], found_send.at[ahead], found_recv.at[ahead], ahead
        )

    def settled_copy(mask):
        return pltpu.make_async_remote_copy(
            src_ref=settled.at[me],
            dst_ref=settled.at[me],
            send_sem=settled_send.at[mask],
            recv_sem=settled_recv.at[mask],
            device_id={"mp": peers[mask]},
            device_id_type=pl.DeviceIdType.MESH,
        )

    def moved(t, j):
        total = offsets_ref[0, j]
        for s in range(1, STEPS):
            total = total + jnp.where(s <= t, offsets_ref[s, j], 0)
        return lax.rem(total, holders)

    bits = []
    bit = shards // 2
    while bit:
        bits.append(bit)
        bit //= 2
    orders = [bits, [bits[1], bits[0]] + bits[2:]]
    half = rows // 2
    masks = sorted(range(1, shards), key=lambda mask: (mask.bit_count(), mask))

    def source(mask):
        return me if mask == 0 else peers[mask]

    def hop(slot, g, s, mask, via):
        block = gath.at[slot, g, source(mask), pl.ds(s * half, half)]
        return pltpu.make_async_remote_copy(
            src_ref=block,
            dst_ref=block,
            send_sem=send_sem.at[g, s, mask ^ via],
            recv_sem=recv_sem.at[g, s, mask ^ via],
            device_id={"mp": peers[via]},
            device_id_type=pl.DeviceIdType.MESH,
        )

    def forward(slot, g, s, mask):
        order = orders[s]
        last = max([order.index(bit) for bit in order if mask & bit], default=-1)
        for via in order[last + 1 :]:
            hop(slot, g, s, mask, via).start()

    def arriving(slot, g, s, mask):
        block = gath.at[slot, g, source(mask), pl.ds(s * half, half)]
        return pltpu.make_async_remote_copy(
            src_ref=block,
            dst_ref=block,
            send_sem=send_sem.at[g, s, mask],
            recv_sem=recv_sem.at[g, s, mask],
            device_id={"mp": peers[mask]},
            device_id_type=pl.DeviceIdType.MESH,
        )

    def launch(g, slot):
        here = pl.ds(g * rows, rows)
        gath[slot, g, me] = carried[here, :].astype(jnp.bfloat16)
        for s in range(2):
            forward(slot, g, s, 0)

    def stat_copy(g, mask):
        return pltpu.make_async_remote_copy(
            src_ref=stats.at[g, 0],
            dst_ref=stats.at[g, mask],
            send_sem=stat_send.at[g, mask],
            recv_sem=stat_recv.at[g, mask],
            device_id={"mp": peers[mask]},
            device_id_type=pl.DeviceIdType.MESH,
        )

    def multiply(g, rows_in, start, depth, first):
        for part in range(3):
            term = jnp.dot(
                rows_in, weight[part, pl.ds(start, depth), :], preferred_element_type=jnp.float32
            )
            if first:
                parts[g, part] = term
            else:
                parts[g, part] += term

    early = [(s, orders[s][0]) for s in range(2)]

    def relay(slot, g):
        for s, mask in early:
            arriving(slot, g, s, mask).wait_recv()
            forward(slot, g, s, mask)

    def gather_and_multiply(t, slot, g):
        multiply(g, embedded[t, pl.ds(g * rows, rows), :], 0, HID, True)
        for mask in [0] + masks:
            if mask:
                for s in range(2):
                    if (s, mask) not in early:
                        arriving(slot, g, s, mask).wait_recv()
                        forward(slot, g, s, mask)
            start = pl.multiple_of(HID + source(mask) * share, share)
            multiply(g, gath[slot, g, source(mask)], start, share, False)
        sums = jnp.zeros((rows, 128), jnp.float32)
        squares = jnp.zeros((rows, 128), jnp.float32)
        for part in range(3):
            for column in range(0, share, 128):
                piece = parts[g, part, :, pl.ds(column, 128)]
                sums = sums + piece
                squares = squares + piece * piece
        stats[g, 0, 0:1, :] = jnp.sum(sums.T, axis=0, keepdims=True)
        stats[g, 0, 1:2, :] = jnp.sum(squares.T, axis=0, keepdims=True)
        for mask in masks:
            stat_copy(g, mask).start()

    def renew(t, slot, g):
        for mask in masks:
            stat_copy(g, mask).wait()
        total = jnp.sum(stats[g], axis=0) / (3 * share * shards)
        average = jnp.broadcast_to(total[0:1], (128, rows)).T
        square = jnp.broadcast_to(total[1:2], (128, rows)).T
        inverse = lax.rsqrt(square - average * average + 1e-05)
        here = pl.ds(g * rows, rows)
        alive = horizon[here, :] > WSTART + t
        for column in range(0, share, 128):
            where = pl.ds(column, 128)
            normed = [(parts[g, part, :, where] - average) * inverse for part in range(3)]
            reset_gate = jax.nn.sigmoid(normed[0])
            candidate = jnp.tanh(reset_gate * normed[1])
            update = jax.nn.sigmoid(normed[2] - 1.0)
            before = carried[here, where]
            renewed = update * candidate + (1.0 - update) * before
            carried[here, where] = jnp.where(alive, renewed, before)
        for s in range(2):
            for mask in masks:
                arriving(slot, g, s, mask).wait_send()

    def leave(g):
        for b in range(group_blocks):
            for k in range(holders):
                start = g * rows + b * block_rows + k * piece
                leaving[g, k, b] = carried[pl.ds(start, piece), :].astype(jnp.bfloat16)
        for ahead in range(1, holders):
            leave_copy(g, ahead).start()
        passing[g, place] = leaving[g, place]

    def route(g):
        for ahead in range(1, holders):
            leave_copy(g, ahead).wait()
        for d in range(holders):
            for b in range(group_blocks):
                holder = lax.rem(d + holders - moved(STEPS - 1, g * group_blocks + b), holders)
                taken = passing[g, 0, b]
                for h in range(1, holders):
                    taken = jnp.where(holder == h, passing[g, h, b], taken)
                routed[g, d, b] = taken
        for ahead in range(1, holders):
            route_copy(g, ahead).start()
        landed[g, place] = routed[g, place]

    def land(g):
        for ahead in range(1, holders):
            route_copy(g, ahead).wait()
        for b in range(group_blocks):
            for k in range(holders):
                start = g * rows + b * block_rows + k * piece
                final_ref[pl.ds(start, piece), :] = landed[g, k, b].astype(jnp.float32)

    def pack(t):
        top = draws[t].astype(jnp.float32)
        low = jnp.broadcast_to(
            actions_ref[t : t + 1, :].astype(jnp.float32), (PACKED - GROUPS, rows_here)
        )
        packed[place, t] = jnp.concatenate([top, low], axis=0).astype(jnp.bfloat16)
        for ahead in range(1, holders):
            pack_copy(t, ahead, place).start()

    class_row = lax.broadcasted_iota(jnp.int32, (1, GROUPS * CLASSES), 1) % CLASSES
    class_row = class_row.astype(jnp.float32)

    def embed(t):
        for ahead in range(1, holders):
            pack_copy(t, ahead, place).wait()
        block = lax.broadcasted_iota(jnp.int32, (PACKED, rows_here), 1) // block_rows
        holder = jnp.zeros((PACKED, rows_here), jnp.int32)
        for j in range(BLK_DEV):
            holder = jnp.where(block == j, lax.rem(place + moved(t, j), holders), holder)
        home = packed[0, t].astype(jnp.float32)
        for h in range(1, holders):
            home = jnp.where(holder == h, packed[h, t].astype(jnp.float32), home)
        tall = jnp.concatenate([home, jnp.zeros((LANES - PACKED, rows_here), jnp.float32)], axis=0)
        flat = tall.T
        classes_of[t] = flat.astype(jnp.bfloat16)
        for start in range(0, rows_here, LANES):
            here = pl.ds(start, LANES)
            low = classes_of[t, here, :]
            hot = (product(low, spread[...]) == class_row).astype(jnp.bfloat16)
            chosen = low[:, GROUPS : GROUPS + 1].astype(jnp.float32)
            action = lax.broadcasted_iota(jnp.int32, (LANES, LANES), 1).astype(jnp.float32)
            hot_action = (action == chosen).astype(jnp.bfloat16)
            pre = product(hot, stoch[...]) + product(hot_action, act[...])
            embedded[t, here, :] = jax.nn.silu(normed_rows(pre)).astype(jnp.bfloat16)

    def take_own(t, slot):
        first = me * own_rows
        g = first // rows
        within = pl.ds(pl.multiple_of(lax.rem(first, rows), own_rows), own_rows)
        for mask in range(shards):
            start = pl.multiple_of(source(mask) * share, share)
            own_states[pl.ds(pl.multiple_of(t * own_rows, own_rows), own_rows), pl.ds(start, share)] = (
                gath[slot, g, source(mask), within, :]
            )

    def judge():
        wide[...] = product(own_states[...], prior[...])
        hidden[...] = jax.nn.silu(normed_rows(wide[...])).astype(jnp.bfloat16)

    def conclude():
        first = pl.ds(pl.multiple_of(me * own_rows, own_rows), own_rows)
        for t in range(STEPS):
            own_classes[pl.ds(t * own_rows, own_rows), :] = classes_of[t, first, :]
        wide[...] = jnp.exp(5.0 * jnp.tanh(product(hidden[...], logit[...]) / 5.0))
        exponent = wide[...]
        hot = product(own_classes[...], spread[...]) == class_row
        high = exponent.astype(jnp.bfloat16)
        low = (exponent - high.astype(jnp.float32)).astype(jnp.bfloat16)
        none = jnp.zeros_like(high)
        sums = product_nt(high, spread[...]) + product_nt(low, spread[...])
        taken = product_nt(jnp.where(hot, high, none), spread[...]) + product_nt(
            jnp.where(hot, low, none), spread[...]
        )
        lane = lax.broadcasted_iota(jnp.int32, (padded, LANES), 1)
        sums = jnp.where(lane < GROUPS, sums, 1.0)
        chances = jnp.where(lane < GROUPS, 0.99 * taken / sums + 0.01 / CLASSES, 1.0)
        log_prob = jnp.sum(jnp.log(chances), axis=-1, keepdims=True)
        heads = product(hidden[...], head_ref[...])
        living = [
            (horizon[first, :] > WSTART + t).astype(jnp.float32) for t in range(STEPS)
        ]
        if STEPS * own_rows < padded:
            living.append(jnp.zeros((padded - STEPS * own_rows, LANES), jnp.float32))
        living = jnp.concatenate(living, axis=0)
        results = jnp.where(
            lane == 0,
            log_prob,
            jnp.where(lane == 1, heads[:, 0:1], jax.nn.sigmoid(heads[:, 1:2])),
        )
        found[place] = (results * living).T[0:8, :]
        for ahead in range(1, holders):
            found_copy(ahead).start()

    def settle():
        for ahead in range(1, holders):
            found_copy(ahead).wait()
        j = (me * own_rows) // block_rows
        lane = lax.broadcasted_iota(jnp.int32, (8, padded), 1) // own_rows
        mine = jnp.zeros((8, padded), jnp.float32)
        for t in range(STEPS):
            holder = lax.rem(place + holders - moved(t, j), holders)
            mine = jnp.where(lane == t, found[holder], mine)
        settled[me] = mine
        for mask in masks:
            settled_copy(mask).start()

    def publish():
        for mask in masks:
            settled_copy(mask).wait()
        lane = lax.broadcasted_iota(jnp.int32, (8, LANES), 1) // own_rows
        fit = LANES // own_rows
        for start in range(0, rows_here, LANES):
            for t in range(STEPS):
                line = jnp.zeros((8, LANES), jnp.float32)
                for k in range(fit):
                    amount = ((k - t) * own_rows) % LANES
                    whole = settled[start // own_rows + k]
                    if amount:
                        whole = pltpu.roll(whole, amount, 1)
                    line = jnp.where(lane == k, whole, line)
                where = pl.ds(start, LANES)
                log_prob_ref[t : t + 1, where] = line[0:1]
                reward_ref[t : t + 1, where] = line[1:2]
                continuation_ref[t : t + 1, where] = line[2:3]

    for k in range(tasks_here):
        horizon[pl.ds(k * task_rows, task_rows), :] = jnp.full(
            (task_rows, LANES), horizons_ref[place * tasks_here + k], jnp.int32
        )
    group_of = lax.broadcasted_iota(jnp.int32, (LANES, GROUPS * CLASSES), 1) // CLASSES
    spread[...] = (
        group_of == lax.broadcasted_iota(jnp.int32, (LANES, GROUPS * CLASSES), 0)
    ).astype(jnp.bfloat16)
    act[...] = jnp.concatenate(
        [act_ref[...].astype(jnp.float32), jnp.zeros((LANES - ACTS, HID), jnp.float32)], axis=0
    ).astype(jnp.bfloat16)
    if STEPS * own_rows < padded:
        own_states[...] = jnp.zeros_like(own_states)
        own_classes[...] = jnp.zeros_like(own_classes)
    fetches[0].wait()
    fetches[1].wait()
    pl.semaphore_wait(barrier, shards - 1 + holders - 1)
    for g in range(groups):
        launch(g, 0)
    for t in range(STEPS):
        pack(t)
    for g in range(groups):
        relay(0, g)
    fetches[2].wait()

    def embed_step(t, _):
        embed(t)
        return 0

    lax.fori_loop(0, STEPS, embed_step, 0)
    fetches[3].wait()
    fetches[4].start()
    fetches[5].start()

    def step(t, _):
        slot = lax.rem(t, 2)
        going = t < STEPS - 1
        gather_and_multiply(t, slot, 0)
        pl.when(t > 0)(functools.partial(relay, slot, 1))
        renew(t, slot, 0)
        pl.when(going)(functools.partial(launch, 0, 1 - slot))
        pl.when(t == STEPS - 1)(functools.partial(leave, 0))
        gather_and_multiply(t, slot, 1)
        take_own(t, slot)

        @pl.when(going)
        def _():
            relay(1 - slot, 0)
            renew(t, slot, 1)
            launch(1, 1 - slot)

        return 0

    lax.fori_loop(0, STEPS, step, 0)
    fetches[4].wait()
    judge()
    route(0)
    renew(STEPS - 1, (STEPS - 1) % 2, 1)
    leave(1)
    fetches[5].wait()
    conclude()
    route(1)
    land(0)
    settle()
    land(1)
    publish()


def window(deter, draws, actions, horizons, offsets, stoch, act, weight, prior, logit, head):
    holders = lax.axis_size("task")
    shards = lax.axis_size("mp")
    rows_here, share = deter.shape
    groups = 2
    rows = rows_here // groups
    own_rows = rows_here // shards
    padded = max(STEPS * own_rows, LANES)
    piece = rows_here // BLK_DEV // holders
    vmem = pl.BlockSpec(memory_space=pltpu.VMEM)
    smem = pl.BlockSpec(memory_space=pltpu.SMEM)
    hbm = pl.BlockSpec(memory_space=pl.ANY)
    dma = pltpu.SemaphoreType.DMA
    low = jnp.bfloat16
    full = jnp.float32
    line = jax.ShapeDtypeStruct((STEPS, rows_here), full)
    moving = (groups, holders, BLK_DEV // groups, piece, share)
    return pl.pallas_call(
        functools.partial(window_kernel, holders, shards, groups, rows, share),
        out_shape=(line, line, line, jax.ShapeDtypeStruct((rows_here, share), full)),
        in_specs=[smem, smem, vmem, vmem, vmem, hbm, hbm, hbm, hbm, hbm, hbm],
        out_specs=(vmem, vmem, vmem, vmem),
        scratch_shapes=[
            pltpu.VMEM((rows_here, share), full),
            pltpu.VMEM(draws.shape, jnp.int32),
            pltpu.VMEM((LANES, HID), low),
            pltpu.VMEM(stoch.shape, low),
            pltpu.VMEM(weight.shape, low),
            pltpu.VMEM(prior.shape, low),
            pltpu.VMEM(logit.shape, low),
            pltpu.VMEM((holders, STEPS, PACKED, rows_here), low),
            pltpu.VMEM((LANES, GROUPS * CLASSES), low),
            pltpu.VMEM((STEPS, rows_here, LANES), low),
            pltpu.VMEM((STEPS, rows_here, HID), low),
            pltpu.VMEM((rows_here, LANES), jnp.int32),
            pltpu.VMEM((padded, shards * share), low),
            pltpu.VMEM((padded, LANES), low),
            pltpu.VMEM((padded, HID), full),
            pltpu.VMEM((padded, HID), low),
            pltpu.VMEM((2, groups, shards, rows, share), low),
            pltpu.VMEM((groups, 3, rows, share), full),
            pltpu.VMEM((groups, shards, 2, rows), full),
            pltpu.VMEM(moving, low),
            pltpu.VMEM(moving, low),
            pltpu.VMEM(moving, low),
            pltpu.VMEM(moving, low),
            pltpu.VMEM((holders, 8, padded), full),
            pltpu.VMEM((shards, 8, padded), full),
            dma((6,)),
            dma((groups, 2, shards)),
            dma((groups, 2, shards)),
            dma((groups, shards)),
            dma((groups, shards)),
            dma((STEPS, holders)),
            dma((STEPS, holders)),
            dma((groups, holders)),
            dma((groups, holders)),
            dma((groups, holders)),
            dma((groups, holders)),
            dma((holders,)),
            dma((holders,)),
            dma((shards,)),
            dma((shards,)),
        ],
        compiler_params=pltpu.CompilerParams(
            collective_id=0, has_side_effects=True, vmem_limit_bytes=62 * 1024 * 1024
        ),
    )(horizons, offsets, actions, act, head, deter, draws, stoch, weight, prior, logit)


def on_device(
    deter,
    draws,
    actions,
    horizons,
    offsets,
    embed_stoch,
    embed_act,
    gru_weight,
    prior_weight,
    logit_weight,
    head_weight,
):
    return window(
        deter,
        draws,
        actions,
        horizons,
        offsets,
        embed_stoch,
        embed_act,
        jnp.transpose(gru_weight, (1, 0, 2)),
        prior_weight,
        logit_weight,
        head_weight,
    )


def solution(mesh):
    in_specs = (
        P("task", "mp"),
        P(None, None, "task"),
        P(None, "task"),
        P(),
        P(),
        P(),
        P(),
        P(None, None, "mp"),
        P(),
        P(),
        P(),
    )
    out_specs = (P(None, "task"), P(None, "task"), P(None, "task"), P("task", "mp"))
    return jax.shard_map(
        on_device, mesh=mesh, in_specs=in_specs, out_specs=out_specs, check_vma=False
    )
```

```python
import functools

import jax
import jax.numpy as jnp
from jax import lax
from jax.experimental import pallas as pl
from jax.experimental.pallas import tpu as pltpu
from jax.sharding import PartitionSpec as P

HID = 1024
GROUPS = 32
CLASSES = 32
ACTS = 18
TASKS = 64
BLK_DEV = 4
STEPS = 4
WSTART = 16
LANES = 128
PACKED = 40
CUTS = 4


def normed_rows(values):
    entries = values.shape[-1]
    average = jnp.sum(values, axis=-1, keepdims=True) / entries
    squares = jnp.sum(values * values, axis=-1, keepdims=True) / entries
    return (values - average) * lax.rsqrt(squares - average * average + 1e-05)


def product(rows_in, weight):
    return jnp.dot(rows_in, weight, preferred_element_type=jnp.float32)


def product_nt(rows_in, weight):
    return lax.dot_general(
        rows_in, weight, (((1,), (1,)), ((), ())), preferred_element_type=jnp.float32
    )


def flipped(index, mask):
    bit = 1
    while bit <= mask:
        if mask & bit:
            index = index + bit * (1 - 2 * ((index // bit) % 2))
        bit *= 2
    return index


def window_kernel(
    holders,
    shards,
    groups,
    rows,
    share,
    horizons_ref,
    offsets_ref,
    actions_ref,
    act_ref,
    head_ref,
    deter_ref,
    draws_ref,
    stoch_ref,
    weight_ref,
    prior_ref,
    logit_ref,
    lines_ref,
    landed,
    carried,
    draws,
    act,
    stoch,
    weight,
    prior,
    logit,
    packed,
    spread,
    classes_of,
    embedded,
    horizon,
    own_states,
    own_classes,
    wide,
    hidden,
    gath,
    parts,
    stats,
    leaving,
    passing,
    routed,
    found,
    settled,
    fetch_sem,
    send_sem,
    recv_sem,
    stat_send,
    stat_recv,
    pack_send,
    pack_recv,
    leave_send,
    leave_recv,
    route_send,
    route_recv,
    found_send,
    found_recv,
    settled_send,
    settled_recv,
):
    me = lax.axis_index("mp")
    place = lax.axis_index("task")
    peers = {mask: flipped(me, mask) for mask in range(1, shards)}
    rows_here = groups * rows
    block_rows = rows_here // BLK_DEV
    group_blocks = BLK_DEV // groups
    piece = block_rows // holders
    own_rows = rows_here // shards
    padded = own_states.shape[0]
    tasks_here = TASKS // holders
    task_rows = rows_here // tasks_here

    def fetch(k, source_ref, target):
        return pltpu.make_async_copy(source_ref, target, fetch_sem.at[k])

    fetches = [
        fetch(0, draws_ref, draws),
        fetch(1, deter_ref, carried),
        fetch(2, stoch_ref, stoch),
        fetch(3, weight_ref, weight),
        fetch(4, prior_ref, prior),
        fetch(5, logit_ref, logit),
    ]
    for k in range(4):
        fetches[k].start()
    barrier = pltpu.get_barrier_semaphore()

    def ahead_of(ahead):
        return lax.rem(place + ahead, holders)

    for mask in range(1, shards):
        pl.semaphore_signal(
            barrier,
            inc=1,
            device_id={"mp": peers[mask]},
            device_id_type=pl.DeviceIdType.MESH,
        )
    for ahead in range(1, holders):
        pl.semaphore_signal(
            barrier,
            inc=1,
            device_id={"task": ahead_of(ahead)},
            device_id_type=pl.DeviceIdType.MESH,
        )

    def across(source_ref, target_ref, send, recv, ahead):
        return pltpu.make_async_remote_copy(
            src_ref=source_ref,
            dst_ref=target_ref,
            send_sem=send,
            recv_sem=recv,
            device_id={"task": ahead_of(ahead)},
            device_id_type=pl.DeviceIdType.MESH,
        )

    def pack_copy(t, ahead, slot):
        return across(
            packed.at[place, t],
            packed.at[slot, t],
            pack_send.at[t, ahead],
            pack_recv.at[t, ahead],
            ahead,
        )

    def leave_copy(j, ahead):
        return across(
            leaving.at[j, ahead_of(ahead)],
            passing.at[j, place],
            leave_send.at[j, ahead],
            leave_recv.at[j, ahead],
            ahead,
        )

    def route_copy(j, ahead):
        return across(
            routed.at[j, ahead_of(ahead)],
            landed.at[j, place],
            route_send.at[j, ahead],
            route_recv.at[j, ahead],
            ahead,
        )

    def found_copy(ahead):
        return across(
            found.at[place], found.at[place], found_send.at[ahead], found_recv.at[ahead], ahead
        )

    def settled_copy(mask):
        return pltpu.make_async_remote_copy(
            src_ref=settled.at[me],
            dst_ref=settled.at[me],
            send_sem=settled_send.at[mask],
            recv_sem=settled_recv.at[mask],
            device_id={"mp": peers[mask]},
            device_id_type=pl.DeviceIdType.MESH,
        )

    def moved(t, j):
        total = offsets_ref[0, j]
        for s in range(1, STEPS):
            total = total + jnp.where(s <= t, offsets_ref[s, j], 0)
        return lax.rem(total, holders)

    bits = []
    bit = shards // 2
    while bit:
        bits.append(bit)
        bit //= 2
    orders = [bits, [bits[1], bits[0]] + bits[2:]]
    size = rows // CUTS
    masks = sorted(range(1, shards), key=lambda mask: (mask.bit_count(), mask))

    def source(mask):
        return me if mask == 0 else peers[mask]

    def hop(slot, g, s, mask, via):
        block = gath.at[slot, g, source(mask), pl.ds(s * size, size)]
        return pltpu.make_async_remote_copy(
            src_ref=block,
            dst_ref=block,
            send_sem=send_sem.at[g, s, mask ^ via],
            recv_sem=recv_sem.at[g, s, mask ^ via],
            device_id={"mp": peers[via]},
            device_id_type=pl.DeviceIdType.MESH,
        )

    def forward(slot, g, s, mask):
        order = orders[s % 2]
        last = max([order.index(bit) for bit in order if mask & bit], default=-1)
        for via in order[last + 1 :]:
            hop(slot, g, s, mask, via).start()

    def arriving(slot, g, s, mask):
        block = gath.at[slot, g, source(mask), pl.ds(s * size, size)]
        return pltpu.make_async_remote_copy(
            src_ref=block,
            dst_ref=block,
            send_sem=send_sem.at[g, s, mask],
            recv_sem=recv_sem.at[g, s, mask],
            device_id={"mp": peers[mask]},
            device_id_type=pl.DeviceIdType.MESH,
        )

    def launch(g, slot):
        here = pl.ds(g * rows, rows)
        gath[slot, g, me] = carried[here, :].astype(jnp.bfloat16)
        for s in range(CUTS):
            forward(slot, g, s, 0)

    def stat_copy(g, mask):
        return pltpu.make_async_remote_copy(
            src_ref=stats.at[g, 0],
            dst_ref=stats.at[g, mask],
            send_sem=stat_send.at[g, mask],
            recv_sem=stat_recv.at[g, mask],
            device_id={"mp": peers[mask]},
            device_id_type=pl.DeviceIdType.MESH,
        )

    def multiply(g, rows_in, start, depth, first):
        for part in range(3):
            term = jnp.dot(
                rows_in, weight[part, pl.ds(start, depth), :], preferred_element_type=jnp.float32
            )
            if first:
                parts[g, part] = term
            else:
                parts[g, part] += term

    early = [(s, orders[s % 2][0]) for s in range(CUTS)]

    near = [mask for mask in masks if mask % 2 == 0 and mask.bit_count() == 1]
    far = [mask for mask in masks if mask % 2 == 0 and mask.bit_count() > 1]

    def relay(slot, g):
        for s, mask in early:
            arriving(slot, g, s, mask).wait_recv()
            forward(slot, g, s, mask)

    def gather_and_multiply(t, slot, g):
        def arrive(mask):
            for s in range(CUTS):
                if (s, mask) not in early:
                    arriving(slot, g, s, mask).wait_recv()
                    forward(slot, g, s, mask)

        def take(mask):
            start = pl.multiple_of(HID + source(mask) * share, share)
            multiply(g, gath[slot, g, source(mask)], start, share, False)

        for mask in near:
            arrive(mask)
        multiply(g, embedded[t, pl.ds(g * rows, rows), :], 0, HID, True)
        take(0)
        arrive(1)
        take(1)
        for mask in near[:-1]:
            take(mask)
        for mask in far:
            arrive(mask)
        take(near[-1])
        rest = [mask for mask in masks if mask % 2 and mask > 1]
        for mask in rest[:-1]:
            arrive(mask)
            take(mask)
        for mask in far:
            take(mask)
        arrive(rest[-1])
        take(rest[-1])
        sums = jnp.zeros((rows, 128), jnp.float32)
        squares = jnp.zeros((rows, 128), jnp.float32)
        for part in range(3):
            for column in range(0, share, 128):
                piece = parts[g, part, :, pl.ds(column, 128)]
                sums = sums + piece
                squares = squares + piece * piece
        stats[g, 0, 0:1, :] = jnp.sum(sums.T, axis=0, keepdims=True)
        stats[g, 0, 1:2, :] = jnp.sum(squares.T, axis=0, keepdims=True)
        for mask in masks:
            stat_copy(g, mask).start()

    def renew(t, slot, g):
        for mask in masks:
            stat_copy(g, mask).wait()
        total = jnp.sum(stats[g], axis=0) / (3 * share * shards)
        average = jnp.broadcast_to(total[0:1], (128, rows)).T
        square = jnp.broadcast_to(total[1:2], (128, rows)).T
        inverse = lax.rsqrt(square - average * average + 1e-05)
        here = pl.ds(g * rows, rows)
        alive = horizon[here, :] > WSTART + t
        for column in range(0, share, 128):
            where = pl.ds(column, 128)
            normed = [(parts[g, part, :, where] - average) * inverse for part in range(3)]
            reset_gate = jax.nn.sigmoid(normed[0])
            candidate = jnp.tanh(reset_gate * normed[1])
            update = jax.nn.sigmoid(normed[2] - 1.0)
            before = carried[here, where]
            renewed = update * candidate + (1.0 - update) * before
            carried[here, where] = jnp.where(alive, renewed, before)
        for s in range(CUTS):
            for mask in masks:
                arriving(slot, g, s, mask).wait_send()

    def leave(j):
        for k in range(holders):
            start = j * block_rows + k * piece
            leaving[j, k] = carried[pl.ds(start, piece), :].astype(jnp.bfloat16)
        for ahead in range(1, holders):
            leave_copy(j, ahead).start()
        passing[j, place] = leaving[j, place]

    def leave_group(g):
        for j in range(g * group_blocks, (g + 1) * group_blocks):
            leave(j)

    def route(j):
        for ahead in range(1, holders):
            leave_copy(j, ahead).wait()
        for d in range(holders):
            holder = lax.rem(d + holders - moved(STEPS - 1, j), holders)
            taken = passing[j, 0]
            for h in range(1, holders):
                taken = jnp.where(holder == h, passing[j, h], taken)
            routed[j, d] = taken
        for ahead in range(1, holders):
            route_copy(j, ahead).start()
        landed[j, place] = routed[j, place]

    def land(j):
        for ahead in range(1, holders):
            route_copy(j, ahead).wait()

    def pack(t):
        top = draws[t].astype(jnp.float32)
        low = jnp.broadcast_to(
            actions_ref[t : t + 1, :].astype(jnp.float32), (PACKED - GROUPS, rows_here)
        )
        packed[place, t] = jnp.concatenate([top, low], axis=0).astype(jnp.bfloat16)
        for ahead in range(1, holders):
            pack_copy(t, ahead, place).start()

    class_row = lax.broadcasted_iota(jnp.int32, (1, GROUPS * CLASSES), 1) % CLASSES
    class_row = class_row.astype(jnp.float32)

    def embed(t):
        for ahead in range(1, holders):
            pack_copy(t, ahead, place).wait()
        block = lax.broadcasted_iota(jnp.int32, (PACKED, rows_here), 1) // block_rows
        holder = jnp.zeros((PACKED, rows_here), jnp.int32)
        for j in range(BLK_DEV):
            holder = jnp.where(block == j, lax.rem(place + moved(t, j), holders), holder)
        home = packed[0, t].astype(jnp.float32)
        for h in range(1, holders):
            home = jnp.where(holder == h, packed[h, t].astype(jnp.float32), home)
        tall = jnp.concatenate([home, jnp.zeros((LANES - PACKED, rows_here), jnp.float32)], axis=0)
        flat = tall.T
        classes_of[t] = flat.astype(jnp.bfloat16)
        for start in range(0, rows_here, LANES):
            here = pl.ds(start, LANES)
            low = classes_of[t, here, :]
            hot = (product(low, spread[...]) == class_row).astype(jnp.bfloat16)
            chosen = low[:, GROUPS : GROUPS + 1].astype(jnp.float32)
            action = lax.broadcasted_iota(jnp.int32, (LANES, LANES), 1).astype(jnp.float32)
            hot_action = (action == chosen).astype(jnp.bfloat16)
            pre = product(hot, stoch[...]) + product(hot_action, act[...])
            embedded[t, here, :] = jax.nn.silu(normed_rows(pre)).astype(jnp.bfloat16)

    def take_own(t, slot):
        first = me * own_rows
        g = first // rows
        within = pl.ds(pl.multiple_of(lax.rem(first, rows), own_rows), own_rows)
        for mask in range(shards):
            start = pl.multiple_of(source(mask) * share, share)
            own_states[pl.ds(pl.multiple_of(t * own_rows, own_rows), own_rows), pl.ds(start, share)] = (
                gath[slot, g, source(mask), within, :]
            )

    def judge():
        wide[...] = product(own_states[...], prior[...])
        hidden[...] = jax.nn.silu(normed_rows(wide[...])).astype(jnp.bfloat16)

    def conclude():
        first = pl.ds(pl.multiple_of(me * own_rows, own_rows), own_rows)
        for t in range(STEPS):
            own_classes[pl.ds(t * own_rows, own_rows), :] = classes_of[t, first, :]
        wide[...] = jnp.exp(5.0 * jnp.tanh(product(hidden[...], logit[...]) / 5.0))
        exponent = wide[...]
        hot = product(own_classes[...], spread[...]) == class_row
        high = exponent.astype(jnp.bfloat16)
        low = (exponent - high.astype(jnp.float32)).astype(jnp.bfloat16)
        none = jnp.zeros_like(high)
        sums = product_nt(high, spread[...]) + product_nt(low, spread[...])
        taken = product_nt(jnp.where(hot, high, none), spread[...]) + product_nt(
            jnp.where(hot, low, none), spread[...]
        )
        lane = lax.broadcasted_iota(jnp.int32, (padded, LANES), 1)
        sums = jnp.where(lane < GROUPS, sums, 1.0)
        chances = jnp.where(lane < GROUPS, 0.99 * taken / sums + 0.01 / CLASSES, 1.0)
        log_prob = jnp.sum(jnp.log(chances), axis=-1, keepdims=True)
        heads = product_nt(hidden[...], head_ref[...])
        living = [
            (horizon[first, :] > WSTART + t).astype(jnp.float32) for t in range(STEPS)
        ]
        if STEPS * own_rows < padded:
            living.append(jnp.zeros((padded - STEPS * own_rows, LANES), jnp.float32))
        living = jnp.concatenate(living, axis=0)
        results = jnp.where(
            lane == 0,
            log_prob,
            jnp.where(lane == 1, heads[:, 0:1], jax.nn.sigmoid(heads[:, 1:2])),
        )
        found[place] = (results * living).T[0:8, :]
        for ahead in range(1, holders):
            found_copy(ahead).start()

    def settle():
        for ahead in range(1, holders):
            found_copy(ahead).wait()
        j = (me * own_rows) // block_rows
        lane = lax.broadcasted_iota(jnp.int32, (8, padded), 1) // own_rows
        mine = jnp.zeros((8, padded), jnp.float32)
        for t in range(STEPS):
            holder = lax.rem(place + holders - moved(t, j), holders)
            mine = jnp.where(lane == t, found[holder], mine)
        settled[me] = mine
        for mask in masks:
            settled_copy(mask).start()

    def publish():
        for mask in masks:
            settled_copy(mask).wait()
        lane = lax.broadcasted_iota(jnp.int32, (8, LANES), 1) // own_rows
        fit = LANES // own_rows
        for start in range(0, rows_here, LANES):
            for t in range(STEPS):
                line = jnp.zeros((8, LANES), jnp.float32)
                for k in range(fit):
                    amount = ((k - t) * own_rows) % LANES
                    whole = settled[start // own_rows + k]
                    if amount:
                        whole = pltpu.roll(whole, amount, 1)
                    line = jnp.where(lane == k, whole, line)
                where = pl.ds(start, LANES)
                lines_ref[t, :, where] = line

    for k in range(tasks_here):
        horizon[pl.ds(k * task_rows, task_rows), :] = jnp.full(
            (task_rows, LANES), horizons_ref[place * tasks_here + k], jnp.int32
        )
    group_of = lax.broadcasted_iota(jnp.int32, (LANES, GROUPS * CLASSES), 1) // CLASSES
    spread[...] = (
        group_of == lax.broadcasted_iota(jnp.int32, (LANES, GROUPS * CLASSES), 0)
    ).astype(jnp.bfloat16)
    act[...] = jnp.concatenate(
        [act_ref[...].astype(jnp.float32), jnp.zeros((LANES - ACTS, HID), jnp.float32)], axis=0
    ).astype(jnp.bfloat16)
    if STEPS * own_rows < padded:
        own_states[...] = jnp.zeros_like(own_states)
        own_classes[...] = jnp.zeros_like(own_classes)
    fetches[0].wait()
    fetches[1].wait()
    pl.semaphore_wait(barrier, shards - 1 + holders - 1)
    for g in range(groups):
        launch(g, 0)
    for t in range(STEPS):
        pack(t)
    for g in range(groups):
        relay(0, g)
    fetches[2].wait()

    embed(0)
    fetches[3].wait()
    fetches[4].start()
    fetches[5].start()

    def step(t, _):
        slot = lax.rem(t, 2)
        going = t < STEPS - 1
        gather_and_multiply(t, slot, 0)
        pl.when(t > 0)(functools.partial(relay, slot, 1))
        pl.when(t == 0)(functools.partial(embed, 1))
        pl.when(t == 1)(functools.partial(embed, 2))
        pl.when(t == 2)(functools.partial(embed, 3))
        renew(t, slot, 0)
        pl.when(going)(functools.partial(launch, 0, 1 - slot))
        pl.when(t == STEPS - 1)(functools.partial(leave_group, 0))
        gather_and_multiply(t, slot, 1)
        take_own(t, slot)

        @pl.when(going)
        def _():
            relay(1 - slot, 0)
            renew(t, slot, 1)
            launch(1, 1 - slot)

        return 0

    lax.fori_loop(0, STEPS, step, 0)
    fetches[4].wait()
    judge()
    for j in range(group_blocks):
        route(j)
    renew(STEPS - 1, (STEPS - 1) % 2, 1)
    leave_group(1)
    fetches[5].wait()
    conclude()
    for j in range(group_blocks, BLK_DEV):
        route(j)
    settle()
    publish()
    for j in range(BLK_DEV):
        land(j)


def hand_out_kernel(lines_ref, landed_ref, log_prob_ref, reward_ref, continuation_ref, final_ref):
    blocks, holders, piece, share = landed_ref.shape
    for k, target in enumerate((log_prob_ref, reward_ref, continuation_ref)):
        for t in range(STEPS):
            target[t : t + 1, :] = lines_ref[t, k : k + 1, :]
    for j in range(blocks):
        for k in range(holders):
            start = (j * holders + k) * piece
            final_ref[pl.ds(start, piece), :] = landed_ref[j, k].astype(jnp.float32)


def hand_out(lines, landed):
    blocks, holders, piece, share = landed.shape
    rows_here = blocks * holders * piece
    line = jax.ShapeDtypeStruct((STEPS, rows_here), jnp.float32)
    vmem = pl.BlockSpec(memory_space=pltpu.VMEM)
    return pl.pallas_call(
        hand_out_kernel,
        out_shape=(line, line, line, jax.ShapeDtypeStruct((rows_here, share), jnp.float32)),
        in_specs=[vmem, vmem],
        out_specs=(vmem, vmem, vmem, vmem),
        compiler_params=pltpu.CompilerParams(vmem_limit_bytes=4 * 1024 * 1024),
    )(lines, landed)


def window(deter, draws, actions, horizons, offsets, stoch, act, weight, prior, logit, head):
    holders = lax.axis_size("task")
    shards = lax.axis_size("mp")
    rows_here, share = deter.shape
    groups = 2
    rows = rows_here // groups
    own_rows = rows_here // shards
    padded = max(STEPS * own_rows, LANES)
    piece = rows_here // BLK_DEV // holders
    vmem = pl.BlockSpec(memory_space=pltpu.VMEM)
    smem = pl.BlockSpec(memory_space=pltpu.SMEM)
    hbm = pl.BlockSpec(memory_space=pl.ANY)
    dma = pltpu.SemaphoreType.DMA
    low = jnp.bfloat16
    full = jnp.float32
    moving = (BLK_DEV, holders, piece, share)
    return pl.pallas_call(
        functools.partial(window_kernel, holders, shards, groups, rows, share),
        out_shape=(
            jax.ShapeDtypeStruct((STEPS, 8, rows_here), full),
            jax.ShapeDtypeStruct(moving, low),
        ),
        in_specs=[smem, smem, vmem, vmem, vmem, hbm, hbm, hbm, hbm, hbm, hbm],
        out_specs=(vmem, vmem),
        scratch_shapes=[
            pltpu.VMEM((rows_here, share), full),
            pltpu.VMEM(draws.shape, jnp.int32),
            pltpu.VMEM((LANES, HID), low),
            pltpu.VMEM(stoch.shape, low),
            pltpu.VMEM(weight.shape, low),
            pltpu.VMEM(prior.shape, low),
            pltpu.VMEM(logit.shape, low),
            pltpu.VMEM((holders, STEPS, PACKED, rows_here), low),
            pltpu.VMEM((LANES, GROUPS * CLASSES), low),
            pltpu.VMEM((STEPS, rows_here, LANES), low),
            pltpu.VMEM((STEPS, rows_here, HID), low),
            pltpu.VMEM((rows_here, LANES), jnp.int32),
            pltpu.VMEM((padded, shards * share), low),
            pltpu.VMEM((padded, LANES), low),
            pltpu.VMEM((padded, HID), full),
            pltpu.VMEM((padded, HID), low),
            pltpu.VMEM((2, groups, shards, rows, share), low),
            pltpu.VMEM((groups, 3, rows, share), full),
            pltpu.VMEM((groups, shards, 2, rows), full),
            pltpu.VMEM(moving, low),
            pltpu.VMEM(moving, low),
            pltpu.VMEM(moving, low),
            pltpu.VMEM((holders, 8, padded), full),
            pltpu.VMEM((shards, 8, padded), full),
            dma((6,)),
            dma((groups, CUTS, shards)),
            dma((groups, CUTS, shards)),
            dma((groups, shards)),
            dma((groups, shards)),
            dma((STEPS, holders)),
            dma((STEPS, holders)),
            dma((BLK_DEV, holders)),
            dma((BLK_DEV, holders)),
            dma((BLK_DEV, holders)),
            dma((BLK_DEV, holders)),
            dma((holders,)),
            dma((holders,)),
            dma((shards,)),
            dma((shards,)),
        ],
        compiler_params=pltpu.CompilerParams(
            collective_id=0, has_side_effects=True, vmem_limit_bytes=62 * 1024 * 1024
        ),
    )(horizons, offsets, actions, act, head, deter, draws, stoch, weight, prior, logit)


def on_device(
    deter,
    draws,
    actions,
    horizons,
    offsets,
    embed_stoch,
    embed_act,
    gru_weight,
    prior_weight,
    logit_weight,
    head_weight,
):
    lines, landed = window(
        deter,
        draws,
        actions,
        horizons,
        offsets,
        embed_stoch,
        embed_act,
        jnp.transpose(gru_weight, (1, 0, 2)),
        prior_weight,
        logit_weight,
        jnp.transpose(head_weight),
    )
    return hand_out(lines, landed)


def solution(mesh):
    in_specs = (
        P("task", "mp"),
        P(None, None, "task"),
        P(None, "task"),
        P(),
        P(),
        P(),
        P(),
        P(None, None, "mp"),
        P(),
        P(),
        P(),
    )
    out_specs = (P(None, "task"), P(None, "task"), P(None, "task"), P("task", "mp"))
    return jax.shard_map(
        on_device, mesh=mesh, in_specs=in_specs, out_specs=out_specs, check_vma=False
    )
```
